256 devices in a mesh: batch: 8 (over x, y_lo), seq: 16 (over y_hi, z), head: 2 (over core).
Axes of the slice: x: 4, y: 4 (y_hi: 2, y_lo: 2; y = y_hi * 2 + y_lo), z: 8, core: 2. Of those that a mesh axis runs over, the one named last changes fastest.
Arguments:
- queries: bfloat16 [1, 49152, 2048], P(None, ('batch', 'seq'), 'head'), parts along dimension 1, may hold values from -240 to 240
- keys: bfloat16 [1, 49152, 1024], P(None, ('batch', 'seq'), 'head'), parts along dimension 1, may hold values from -6 to 6
- values: bfloat16 [1, 49152, 1024], P(None, ('batch', 'seq'), 'head'), parts along dimension 1, may hold values from -6 to 6
- exit_layer: int32 [384], P(('batch', 'seq')), parts along dimension 0, may hold values from 0 to 1
- tile_order: int32 [384], P('batch'), parts along dimension 0, may hold values from 0 to 47, each once
Outputs:
- attended: bfloat16 [1, 49152, 2048], P(None, ('batch', 'seq'), 'head'), parts along dimension 1
- live_tiles: int32 [8], P('batch'), parts along dimension 0
The draws below stay inside these ranges and needn't reach their ends.
There are 8 independent parts, one for each index of `batch`. The reference program is written for one: setup_inputs(seed, part) draws one part's arguments, and reference() takes and returns one part's arrays. A program takes and returns all parts, laid end to end along the dimension named above; each array names one. Nothing has to cross between parts.
Inputs may be any that keep to these rules, and one draw needn't show every extreme that they name: Tile t covers tokens t * 128 to t * 128 + 127 of the token dimension; tile_order is a permutation of 0 to 47.
All inputs are finite; a program needn't handle non-finite values.
Results may differ from the reference program's by a relative error of at most 0.0049.
Values may be sent and summed in bfloat16 or wider, within the bound.
No kernel may reach another device: no remote copies, remote signals or barrier semaphores. Data moves between devices by JAX's collectives and lax.ppermute only.
A program may use at most 128 MiB of HBM per device.

```python
import math
import jax
import jax.numpy as jnp
from jax import lax

LAYERS = 1
QH = 8
KVH = 4
HD = 256
TILE = 128
TOKENS = 6144
TILES = 48
KW = 1024


def draw_queries(key, part):
    query_key = jax.random.fold_in(key, 101)
    base = jnp.clip(jax.random.normal(query_key, (LAYERS, TOKENS, QH * HD), jnp.float32), -6.0, 6.0)
    return base.astype(jnp.bfloat16)


def draw_exit_layer(key, part):
    exit_key = jax.random.fold_in(key, 202)
    tile_ids = jnp.arange(TILES, dtype=jnp.int32)
    lowest = tile_ids * LAYERS // TILES
    spread = LAYERS + 1 - lowest
    raw_bits = jax.random.randint(exit_key, (TILES,), 0, 1 << 20, dtype=jnp.int32)
    return (lowest + raw_bits % spread).astype(jnp.int32)


def levels(own_key, shape, pieces, low, largest):
    def one(dim, parts):
        draws = jax.random.uniform(jax.random.fold_in(jax.random.fold_in(own_key, 6), dim), (parts,), jnp.float32, low / len(pieces), largest / len(pieces))
        return jnp.repeat(jnp.exp(draws), shape[dim] // parts).reshape((-1,) + (1,) * (len(shape) - dim - 1))

    gain = one(*pieces[0])
    for cut in pieces[1:]:
        gain = gain * one(*cut)
    return gain


def bell_draw(own_key, shape, width, reach, shards=(), held_as=jnp.bfloat16):
    drawn = width * jax.random.normal(own_key, shape, jnp.float32)
    if shards:
        drawn = drawn * levels(own_key, shape, shards, -0.22, 0.18)
    return jnp.clip(drawn, -reach, reach).astype(held_as)


def setup_inputs(seed: int = 0, part: int = 0) -> dict:
    streams_of = jax.random.split(jax.random.key(seed), 6)
    part_keys = jax.random.split(jax.random.fold_in(streams_of[5], part), 6)
    queries = draw_queries(jax.random.fold_in(jax.random.fold_in(streams_of[5], part), 71), part)
    keys = bell_draw(part_keys[1], (LAYERS, TOKENS, KW), 1.0, 6.0, ((1, 16), (2, 2)))
    values = bell_draw(part_keys[2], (LAYERS, TOKENS, KW), 1.0, 6.0, ((1, 16), (2, 2)))
    exit_layer = draw_exit_layer(jax.random.fold_in(jax.random.fold_in(streams_of[5], part), 71), part)
    tile_order = jax.random.permutation(part_keys[4], TILES).astype(jnp.int32)
    return dict(queries=queries, keys=keys, values=values, exit_layer=exit_layer, tile_order=tile_order)


softcap = 50.0
query_scale = 0.0625


def reference(queries, keys, values, exit_layer, tile_order):
    group_size = QH // KVH
    offsets = jnp.arange(TOKENS, dtype=jnp.int32)
    positions = (tile_order[offsets // TILE] * TILE + offsets % TILE).astype(jnp.int32)
    token_exits = exit_layer[offsets // TILE]
    block_rows = math.gcd(TOKENS, 512)
    outputs = []
    for layer_id in range(LAYERS):
        key_heads = keys[layer_id].reshape(TOKENS, KVH, HD).astype(jnp.float32)
        value_heads = values[layer_id].reshape(TOKENS, KVH, HD).astype(jnp.float32)
        query_blocks = queries[layer_id].reshape(TOKENS // block_rows, block_rows, KVH, group_size, HD)
        query_pos = positions.reshape(TOKENS // block_rows, block_rows)

        def one_block(operands):
            query_block, pos_block = operands
            scores = jnp.einsum("tkgd,skd->kgts", query_block.astype(jnp.float32), key_heads) * query_scale
            allowed = positions[None, :] <= pos_block[:, None]
            weights = jnp.where(allowed[None, None], jnp.exp(softcap * jnp.tanh(scores / softcap)), 0.0)
            denominator = jnp.sum(weights, axis=-1)
            rounded = lax.optimization_barrier(weights.astype(jnp.bfloat16))
            numerator = jnp.einsum("kgts,skd->kgtd", rounded.astype(jnp.float32), value_heads)
            output = numerator / denominator[..., None]
            return jnp.transpose(output, (2, 0, 1, 3)).reshape(block_rows, QH * HD)

        attended_layer = lax.map(one_block, (query_blocks, query_pos)).reshape(TOKENS, QH * HD)
        attended_layer = jnp.where((token_exits > layer_id)[:, None], attended_layer, 0.0)
        outputs.append(attended_layer.astype(jnp.bfloat16))
    live_tiles = jnp.stack([jnp.sum((exit_layer > layer_id).astype(jnp.int32)) for layer_id in range(LAYERS)])
    return jnp.stack(outputs), live_tiles.astype(jnp.int32)
```

```python
import functools
import math

import jax
import jax.numpy as jnp
from jax import lax
from jax.experimental import pallas as pl
from jax.experimental.pallas import tpu as pltpu
from jax.sharding import Mesh
from jax.sharding import PartitionSpec as P

HD = 256
TILE = 128
BATCH_SEQ = ("batch", "seq_0", "seq_1")

softcap = 50.0
query_scale = 0.0625
TO_TANH = query_scale / softcap
TO_EXP2 = softcap * math.log2(math.e)


def attend_kernel(tiles, ring, pieces, sets, first, last, table_ref, *refs):
    refs = list(refs)
    kv_refs = [refs.pop(0) for _ in pieces]
    q_refs = [refs.pop(0) for _ in sets]
    sums_in = [] if first else [(refs.pop(0), refs.pop(0)) for _ in sets]
    if last:
        outs = [refs.pop(0) for _ in sets]
    else:
        sums_out = [(refs.pop(0), refs.pop(0)) for _ in sets]
    total = tiles * 2 * ring
    column = table_ref[total]
    place = table_ref[total + 1]

    def tile_slot(other, offset, i):
        col = 1 - column if other else column
        at = lax.rem(place + (offset + ring), ring)
        return (col * ring + at) * tiles + i

    key_places = [
        [table_ref[tile_slot(other, offset, i)] for i in range(tiles)] for other, offset in pieces
    ]
    rows = 2 * TILE
    ahead = lax.broadcasted_iota(jnp.int32, (TILE, TILE), 1) - lax.broadcasted_iota(
        jnp.int32, (TILE, TILE), 0
    )
    ahead = jnp.concatenate([ahead, ahead], axis=0)

    for s, other in enumerate(sets):
        def one_tile(i, nothing, s=s, other=other):
            here = pl.ds(pl.multiple_of(i * TILE, TILE), TILE)
            q_place = table_ref[tile_slot(other, 0, i)]
            live = table_ref[total + 2 + tiles * int(other) + i] > 0
            lowest = key_places[0][0]
            for places in key_places:
                for place_ in places:
                    lowest = jnp.minimum(lowest, place_)
            wanted = jnp.logical_and(live, lowest <= q_place)

            def read(ref, width):
                return jnp.concatenate([ref[here, :width], ref[here, width:]], axis=0)

            def write(ref, value, width):
                ref[here, :width] = value[:TILE]
                ref[here, width:] = value[TILE:]

            def finish(numerator, denominator):
                divisor = jnp.sum(denominator, axis=1, keepdims=True)
                divisor = jnp.where(divisor > 0.0, divisor, 1.0)
                write(outs[s], (numerator / divisor).astype(jnp.bfloat16), HD)

            @pl.when(wanted)
            def _():
                q2 = read(q_refs[s], HD)
                if first:
                    numerator = jnp.zeros((rows, HD), jnp.float32)
                    denominator = jnp.zeros((rows, TILE), jnp.float32)
                else:
                    numerator = read(sums_in[s][0], HD)
                    denominator = read(sums_in[s][1], TILE)
                for kv_ref, places in zip(kv_refs, key_places):
                    scores = lax.dot_general(
                        q2,
                        kv_ref[:, :HD],
                        (((1,), (1,)), ((), ())),
                        preferred_element_type=jnp.float32,
                    )
                    packed = []
                    for j in range(tiles):
                        part = scores[:, j * TILE : (j + 1) * TILE]
                        weight = jnp.exp2(TO_EXP2 * jnp.tanh(part * TO_TANH))
                        room = (q_place - places[j]) * TILE
                        weight = jnp.where(ahead <= room, weight, 0.0)
                        denominator = denominator + weight
                        packed.append(weight.astype(jnp.bfloat16))
                    numerator = numerator + jnp.dot(
                        jnp.concatenate(packed, axis=1),
                        kv_ref[:, HD:],
                        preferred_element_type=jnp.float32,
                    )
                if last:
                    finish(numerator, denominator)
                else:
                    write(sums_out[s][0], numerator, HD)
                    write(sums_out[s][1], denominator, TILE)

            if first or last:
                @pl.when(jnp.logical_not(wanted))
                def _():
                    if first:
                        write(sums_out[s][0], jnp.zeros((rows, HD), jnp.float32), HD)
                        write(sums_out[s][1], jnp.zeros((rows, TILE), jnp.float32), TILE)
                    else:
                        finish(read(sums_in[s][0], HD), read(sums_in[s][1], TILE))
            return nothing

        lax.fori_loop(0, tiles, one_tile, 0)


def attend(table, ring, pieces, blocks, sets, queries, sums, last, name):
    row_count, width = queries[0].shape
    tiles = row_count // TILE
    first = sums is None
    vmem = pl.BlockSpec(memory_space=pltpu.VMEM)
    smem = pl.BlockSpec(memory_space=pltpu.SMEM)
    operands = [table, *blocks, *queries]
    aliases = {}
    if not first:
        for pair in sums:
            operands.extend(pair)
    if last:
        out_shape = [jax.ShapeDtypeStruct((row_count, width), jnp.bfloat16) for _ in sets]
    else:
        out_shape = []
        for _ in sets:
            out_shape.append(jax.ShapeDtypeStruct((row_count, width), jnp.float32))
            out_shape.append(jax.ShapeDtypeStruct((row_count, 2 * TILE), jnp.float32))
        if not first:
            start = 1 + len(blocks) + len(queries)
            aliases = {start + i: i for i in range(2 * len(sets))}
    keys = sum(b.shape[0] for b in blocks)
    work = len(sets) * row_count * 2 * keys
    out = pl.pallas_call(
        functools.partial(attend_kernel, tiles, ring, pieces, sets, first, last),
        out_shape=out_shape,
        in_specs=[smem] + [vmem] * (len(operands) - 1),
        out_specs=[vmem] * len(out_shape),
        input_output_aliases=aliases,
        compiler_params=pltpu.CompilerParams(vmem_limit_bytes=24 * 1024 * 1024),
        cost_estimate=pl.CostEstimate(
            flops=4 * work * HD, bytes_accessed=4 * work // HD, transcendentals=2 * work
        ),
        name=name,
    )(*operands)
    if last:
        return out
    return [(out[2 * i], out[2 * i + 1]) for i in range(len(sets))]


def body(queries, keys, values, exit_layer, tile_order):
    ring = lax.axis_size("seq_1")
    column = lax.axis_index("seq_0")
    place = lax.axis_index("seq_1")
    swap = [(0, 1), (1, 0)]
    up = [(i, (i + 1) % ring) for i in range(ring)]
    down = [(i, (i - 1) % ring) for i in range(ring)]

    def halves(x):
        half = x.shape[1] // 2
        low, high = x[:, :half], x[:, half:]
        return low, high

    def pick(low, high, which):
        return jnp.where(which == 0, low, high)

    k_low, k_high = halves(keys[0])
    v_low, v_high = halves(values[0])
    q_low, q_high = halves(queries[0])
    kv_low = jnp.concatenate([k_low, v_low], axis=1)
    kv_high = jnp.concatenate([k_high, v_high], axis=1)
    kv_mine = pick(kv_low, kv_high, column)
    kv_theirs = pick(kv_low, kv_high, 1 - column)
    q_mine = pick(q_low, q_high, column)
    q_theirs = pick(q_low, q_high, 1 - column)

    kv_partner = lax.ppermute(kv_theirs, "seq_0", swap)
    q_partner = lax.ppermute(q_theirs, "seq_0", swap)
    exit_partner = lax.ppermute(exit_layer, "seq_0", swap)

    table = jnp.concatenate(
        [tile_order, jnp.stack([column, place]).astype(jnp.int32), exit_layer, exit_partner]
    )

    own = {0: kv_mine}
    other = {0: kv_partner}
    far = ring // 2
    for d in range(1, far + 1):
        own[-d] = lax.ppermute(own[-d + 1], "seq_1", up)
        if d < far:
            other[-d] = lax.ppermute(other[-d + 1], "seq_1", up)
            own[d] = lax.ppermute(own[d - 1], "seq_1", down)
        other[d] = lax.ppermute(other[d - 1], "seq_1", down)

    sets = (False, True)
    q_all = [q_mine, q_partner]
    calls = [[(False, 0), (True, 0)]]
    for d in range(1, far):
        calls.append([(False, -d), (False, d)])
        calls.append([(True, -d), (True, d)])
    sums = None
    for n, call in enumerate(calls):
        blocks = [(other if o else own)[d] for o, d in call]
        sums = attend(table, ring, tuple(call), blocks, sets, q_all, sums, False, f"attend_{n}")
    final = ((False, -far), (True, far))
    blocks = [own[-far], other[far]]
    (out_partner,) = attend(
        table, ring, final, blocks, (True,), q_all[1:], sums[1:], True, "attend_last_partner"
    )
    (out_mine,) = attend(
        table, ring, final, blocks, (False,), q_all[:1], sums[:1], True, "attend_last_mine"
    )
    arrived = lax.ppermute(out_partner, "seq_0", swap)
    live = jnp.repeat(exit_layer > 0, TILE, total_repeat_length=out_mine.shape[0])[:, None]
    low = pick(out_mine, arrived, column)
    high = pick(out_mine, arrived, 1 - column)
    attended = jnp.where(live, jnp.concatenate([low, high], axis=1), 0.0).astype(jnp.bfloat16)

    count = jnp.sum((exit_layer > 0).astype(jnp.int32)) + jnp.sum(
        (exit_partner > 0).astype(jnp.int32)
    )
    count = count[None]
    step = 1
    while step < ring:
        count = count + lax.ppermute(count, "seq_1", [(i, i ^ step) for i in range(ring)])
        step *= 2
    return attended[None], count


def solution(mesh):
    finer = Mesh(
        mesh.devices.reshape(mesh.shape["batch"], 2, 8, mesh.shape["head"]),
        ("batch", "seq_0", "seq_1", "head"),
    )
    return jax.shard_map(
        body,
        mesh=finer,
        in_specs=(
            P(None, BATCH_SEQ, "head"),
            P(None, BATCH_SEQ, "head"),
            P(None, BATCH_SEQ, "head"),
            P(BATCH_SEQ),
            P("batch"),
        ),
        out_specs=(P(None, BATCH_SEQ, "head"), P("batch")),
        check_vma=False,
    )
```
